32 devices in a mesh: dp: 16 (over z, x, core), tp: 2 (over y).
Axes of the slice: x: 2, y: 2, z: 4, core: 2. Of those that a mesh axis runs over, the one named last changes fastest.
Arguments:
- stash_values: bfloat16 [4096, 8192], P(('dp', 'tp')), may hold values from -127 to 127
- stash_scales: bfloat16 [4096, 64], P(('dp', 'tp')), may hold values from 0.001 to 0.13
- value_grad: bfloat16 [4096, 256], P('dp', 'tp'), may hold values from -19 to 19
Outputs:
- clipped_grad: float32 [8192, 256], P('dp', 'tp')
The draws below stay inside these ranges and needn't reach their ends.
All inputs are finite; a program needn't handle non-finite values.
Results may differ from the reference program's by a relative error of at most 0.0019.
Values may be sent and summed in bfloat16 or wider, within the bound.
No kernel may reach another device: no remote copies, remote signals or barrier semaphores. Data moves between devices by JAX's collectives and lax.ppermute only.
A program may use at most 64 MiB of HBM per device.

```python
import math
import jax
import jax.numpy as jnp
from jax import lax

D = 8192
HD = 128
QB = 128
TOK_DEV = 128
KV_HEADS = 2
TOKENS = 4096
N_DP = 16
N_TP = 2


def draw_stash_values(key, part):
    offset_top = min(17, 120 // math.isqrt(math.isqrt(TOKENS)))
    offset_low = 3 * offset_top // 4
    magnitude = jax.random.randint(jax.random.fold_in(key, 18), (D,), offset_low, offset_top + 1)
    sign_draw = 2 * jax.random.randint(jax.random.fold_in(key, 19), (D,), 0, 2) - 1
    noise = jax.random.randint(jax.random.fold_in(key, 17), (TOKENS, D), -110, 111)
    whole = noise + (sign_draw * magnitude)[None, :]
    return whole.astype(jnp.float32).astype(jnp.bfloat16)


def spread_levels(key, count, spread):
    order = jax.random.permutation(jax.random.fold_in(key, 1), count).astype(jnp.float32)
    jitter = jax.random.uniform(jax.random.fold_in(key, 2), (count,), jnp.float32)
    return jnp.exp(spread * (order + jitter) / count - 0.5 * spread)


def draw_stash_scales(key, part):
    blocks = D // QB
    spread = jnp.log(jnp.float32(10.0))
    logs = jax.random.uniform(jax.random.fold_in(key, 34), (TOKENS, blocks), jnp.float32, jnp.log(0.004), jnp.log(0.04))
    base = jnp.exp(logs)
    levels = spread_levels(jax.random.fold_in(key, 31), blocks, spread)
    return (base * levels[None, :]).astype(jnp.bfloat16)


def draw_value_grad(key, part):
    heads = KV_HEADS
    spread = jnp.log(jnp.float32(10.0))
    strength = jnp.float32(1.6)
    noise = jax.random.truncated_normal(jax.random.fold_in(key, 44), -5.4, 5.4, (TOKENS, heads * HD), jnp.float32)
    column_signs = (2 * jax.random.randint(jax.random.fold_in(key, 46), (heads * HD,), 0, 2) - 1).astype(jnp.float32)
    shift = strength * jnp.float32(TOKENS) ** (-0.25) * column_signs
    levels = spread_levels(jax.random.fold_in(key, 41), heads, spread)
    column_levels = jnp.repeat(levels, HD)
    return ((noise + shift[None, :]) * column_levels[None, :]).astype(jnp.bfloat16)


def setup_inputs(seed: int = 0) -> dict:
    streams_of = jax.random.split(jax.random.key(seed), 4)
    return {
        "stash_values": draw_stash_values(jax.random.fold_in(streams_of[3], 71), 0),
        "stash_scales": draw_stash_scales(jax.random.fold_in(streams_of[3], 71), 0),
        "value_grad": draw_value_grad(jax.random.fold_in(streams_of[3], 71), 0),
    }


def reference(stash_values, stash_scales, value_grad):
    width = stash_values.shape[1]
    group = TOK_DEV * N_TP
    columns = value_grad.shape[1]

    def one_group(total, index):
        start = (index * group).astype(jnp.int32)
        values = lax.dynamic_slice_in_dim(stash_values, start, group, 0)
        scales = lax.dynamic_slice_in_dim(stash_scales, start, group, 0)
        grads = lax.dynamic_slice_in_dim(value_grad, start, group, 0)
        blocks = values.astype(jnp.float32).reshape(group, width // QB, QB) * scales.astype(jnp.float32)[:, :, None]
        dequantized = blocks.reshape(group, width).astype(jnp.bfloat16)
        term = jnp.dot(dequantized.astype(jnp.float32).T, grads.astype(jnp.float32), precision=lax.Precision.HIGHEST)
        return (total + term, None)
    start_total = jnp.zeros((width, columns), jnp.float32)
    weight_sum, unused = lax.scan(one_group, start_total, jnp.arange(N_DP, dtype=jnp.int32))
    grad_norm = jnp.sqrt(jnp.sum(weight_sum * weight_sum))
    limit = jnp.sqrt(jnp.float32(width * columns))
    return weight_sum * jnp.minimum(jnp.float32(1.0), limit / grad_norm)
```

```python
import functools

import jax
import jax.numpy as jnp
from jax import lax
from jax.experimental import pallas as pl
from jax.experimental.pallas import tpu as pltpu
from jax.sharding import PartitionSpec as P

AXES = ("dp", "tp")
VMEM = pl.BlockSpec(memory_space=pltpu.VMEM)


def swap(value, count, distance):
    return lax.ppermute(value, AXES, [(i, i ^ distance) for i in range(count)])


def me(n_tp):
    return lax.axis_index("dp") * n_tp + lax.axis_index("tp")


def pack_kernel(n_tp, plane, planes, sub, block, x_ref, s_ref, *outs):
    index = me(n_tp)
    scales = s_ref[...]
    blocks = scales.shape[1]
    lane = lax.broadcasted_iota(jnp.int32, (blocks, sub), 1) // block
    row = lax.broadcasted_iota(jnp.int32, (blocks, sub), 0)
    for k, out in enumerate(outs):
        for n, j in enumerate(planes):
            part = lax.bitwise_xor(index, jnp.int32(j * plane + k))
            pick = (row == lane + part * (sub // block)).astype(jnp.bfloat16)
            spread = jnp.dot(scales, pick, preferred_element_type=jnp.float32)
            values = x_ref[:, pl.ds(pl.multiple_of(part * sub, sub), sub)].astype(jnp.float32)
            out[:, n * sub:(n + 1) * sub] = (values * spread).astype(jnp.bfloat16)


def pack(x, scales, n_tp, plane, planes, sub):
    rows = x.shape[0]
    block = x.shape[1] // scales.shape[1]
    shape = jax.ShapeDtypeStruct((rows, len(planes) * sub), jnp.bfloat16)
    return pl.pallas_call(
        functools.partial(pack_kernel, n_tp, plane, planes, sub, block),
        out_shape=[shape] * plane,
        in_specs=[VMEM] * 2,
        out_specs=[VMEM] * plane,
        cost_estimate=pl.CostEstimate(
            flops=2 * rows * sub * len(planes) * plane,
            bytes_accessed=4 * rows * sub * len(planes) * plane,
            transcendentals=0,
        ),
        name="pack",
    )(x, scales)


def grads_kernel(n_tp, rows, *refs):
    *ins, out = refs
    tp = lax.axis_index("tp")
    hd = ins[0].shape[1]
    for g in range(len(ins) // n_tp):
        for kt in range(n_tp):
            start = pl.multiple_of(lax.bitwise_xor(tp, jnp.int32(kt)) * rows, rows)
            for h in range(n_tp):
                piece = ins[g * n_tp + h][pl.ds(start, rows), :]
                column = (g * n_tp + kt) * rows
                out[h * hd:(h + 1) * hd, column:column + rows] = piece.T


def grads(pieces, n_tp, rows):
    hd = pieces[0].shape[1]
    return pl.pallas_call(
        functools.partial(grads_kernel, n_tp, rows),
        out_shape=jax.ShapeDtypeStruct((n_tp * hd, len(pieces) * rows), jnp.bfloat16),
        in_specs=[VMEM] * len(pieces),
        out_specs=VMEM,
        cost_estimate=pl.CostEstimate(
            flops=len(pieces) * rows * hd * n_tp, bytes_accessed=4 * len(pieces) * rows * hd * n_tp, transcendentals=0
        ),
        name="grads",
    )(*pieces)


def matmul_kernel(sub, n_grads, *refs):
    gt = jnp.concatenate([r[...] for r in refs[:n_grads]], axis=1)
    outs = [r for r in refs if r.shape[0] == gt.shape[0]][n_grads:]
    ins = refs[n_grads:len(refs) - len(outs)]
    x = jnp.concatenate([r[...] for r in ins], axis=0)
    for n, out in enumerate(outs):
        total = jnp.dot(gt, x[:, n * sub:(n + 1) * sub], preferred_element_type=jnp.float32)
        out[...] = total.astype(out.dtype)


def matmul(gts, xs, types, sub):
    columns = gts[0].shape[0]
    tokens = sum(x.shape[0] for x in xs)
    return pl.pallas_call(
        functools.partial(matmul_kernel, sub, len(gts)),
        out_shape=[jax.ShapeDtypeStruct((columns, sub), t) for t in types],
        in_specs=[VMEM] * (len(gts) + len(xs)),
        out_specs=[VMEM] * len(types),
        cost_estimate=pl.CostEstimate(
            flops=2 * columns * tokens * sub * len(types),
            bytes_accessed=2 * tokens * sub * len(types),
            transcendentals=0,
        ),
        name="matmul",
    )(*gts, *xs)


def total_kernel(*refs):
    *ins, own, other, squares = refs
    total = ins[0][...]
    for r in ins[1:]:
        total = total + r[...].astype(jnp.float32)
    half = own.shape[0]
    own[...] = total[:half]
    other[...] = total[half:]
    squared = total * total
    squares[...] = squared.reshape(-1, 8, squared.shape[1]).sum(0)[:, :128] + sum(
        squared.reshape(-1, 8, squared.shape[1]).sum(0)[:, n:n + 128] for n in range(128, squared.shape[1], 128)
    )


def totals(parts):
    columns, sub = parts[0].shape
    half = jax.ShapeDtypeStruct((columns // 2, sub), jnp.float32)
    return pl.pallas_call(
        total_kernel,
        out_shape=[half, half, jax.ShapeDtypeStruct((8, 128), jnp.float32)],
        in_specs=[VMEM] * len(parts),
        out_specs=[VMEM] * 3,
        cost_estimate=pl.CostEstimate(flops=8 * columns * sub, bytes_accessed=8 * columns * sub, transcendentals=0),
        name="totals",
    )(*parts)


def clip_kernel(limit_squared, own, other, *refs):
    *squares, out = refs
    tp = lax.axis_index("tp")
    sub = own.shape[1]
    total = jnp.sum(sum(r[...] for r in squares))
    norm = jnp.sqrt(jnp.full((8, 128), total, jnp.float32))
    factor = jnp.minimum(jnp.float32(1.0), jnp.sqrt(jnp.float32(limit_squared)) / norm)[:1]
    out[pl.ds(pl.multiple_of(tp * sub, sub), sub), :] = own[...].T * factor
    out[pl.ds(pl.multiple_of((1 - tp) * sub, sub), sub), :] = other[...].T * factor


def clip(own, other, squares, limit_squared):
    hd, sub = own.shape
    return pl.pallas_call(
        functools.partial(clip_kernel, limit_squared),
        out_shape=jax.ShapeDtypeStruct((2 * sub, hd), jnp.float32),
        in_specs=[VMEM] * (2 + len(squares)),
        out_specs=VMEM,
        cost_estimate=pl.CostEstimate(flops=4 * hd * sub, bytes_accessed=16 * hd * sub, transcendentals=0),
        name="clip",
    )(own, other, *squares)


def fast_body(inner, stash_values, stash_scales, value_grad):
    n_dp, n_tp = lax.axis_size("dp"), lax.axis_size("tp")
    count = n_dp * n_tp
    plane = inner * n_tp
    depth = count // plane
    rows, width = stash_values.shape
    sub = width // count
    send = functools.partial(swap, count=count)

    far = inner // 2 * n_tp
    near = [value_grad] + [send(value_grad, distance=k) for k in range(1, n_tp)]
    near += [send(value_grad, distance=far + k) for k in range(n_tp)]
    gt = grads(near, n_tp, rows)
    gts = [gt]
    order = list(range(n_tp)) + [far + k for k in range(n_tp)]
    orders = list(order)
    step = n_tp
    while step < far:
        gts += [send(g, distance=step) for g in gts]
        orders += [k ^ step for k in orders]
        step *= 2

    chunks = [tuple(range(depth - 1, 1, -1)), (1, 0)]
    parts = []
    for planes in chunks:
        packed = pack(stash_values, stash_scales, n_tp, plane, planes, sub)
        arrived = [packed[0] if k == 0 else send(packed[k], distance=k) for k in range(plane)]
        types = [jnp.bfloat16 if j else jnp.float32 for j in planes]
        products = matmul(gts, [arrived[k] for k in orders], types, sub)
        parts += [send(q, distance=j * plane) if j else q for j, q in zip(planes, products)]
    own, other, squares = totals(parts[::-1])
    other = send(other, distance=1)

    distance = n_tp
    groups = [(n_tp,), (1, far, far + 1), tuple(j * plane for j in range(1, depth))]
    pieces = [squares]
    for group in groups:
        merged = sum(pieces[1:], pieces[0])
        pieces = [merged] + [send(merged, distance=k) for k in group]
    columns = value_grad.shape[1] * n_tp
    return clip(own, other, pieces, width * columns)


def block_dequantize(values, scales):
    rows = values.shape[0]
    blocks = scales.shape[1]
    scaled = (
        values.astype(jnp.float32).reshape(rows, blocks, values.shape[1] // blocks)
        * scales.astype(jnp.float32)[:, :, None]
    )
    return scaled.reshape(rows, values.shape[1]).astype(jnp.bfloat16)


def body(stash_values, stash_scales, value_grad):
    width = stash_values.shape[1]
    columns = value_grad.shape[1]
    dp_count = lax.axis_size("dp")
    tp_count = lax.axis_size("tp")
    own_tokens = stash_values.shape[0]
    sub_rows = width // (dp_count * tp_count)
    if tp_count == 2 and dp_count == 16 and sub_rows % 256 == 0 and own_tokens % 128 == 0 and columns == 128:
        return fast_body(4, stash_values, stash_scales, value_grad)
    inputs = block_dequantize(stash_values, stash_scales)
    inputs = inputs.reshape(own_tokens, dp_count, tp_count, sub_rows)
    features = lax.all_to_all(inputs, "tp", split_axis=2, concat_axis=0, tiled=True)
    features = features.reshape(own_tokens * tp_count, dp_count * sub_rows)
    all_heads = lax.dot_general(
        features,
        lax.all_gather(value_grad, "tp", axis=1, tiled=True),
        (((0,), (0,)), ((), ())),
        preferred_element_type=jnp.float32,
    )
    summed = lax.psum_scatter(all_heads, "dp", scatter_dimension=0, tiled=True)
    local = lax.all_to_all(summed, "tp", split_axis=1, concat_axis=0, tiled=True)
    total = lax.psum(jnp.sum(summed * summed), ("dp", "tp"))
    limit = jnp.sqrt(jnp.float32(width * columns * lax.axis_size("tp")))
    return local * jnp.minimum(jnp.float32(1.0), limit / jnp.sqrt(total))


def solution(mesh):
    placed = (P(("dp", "tp"), None), P(("dp", "tp"), None), P("dp", "tp"))
    return jax.shard_map(body, mesh=mesh, in_specs=placed, out_specs=P("dp", "tp"), check_vma=False)
```

```python
import functools

import jax
import jax.numpy as jnp
from jax import lax
from jax.experimental import pallas as pl
from jax.experimental.pallas import tpu as pltpu
from jax.sharding import PartitionSpec as P


AXES = ("dp", "tp")
VMEM = pl.BlockSpec(memory_space=pltpu.VMEM)


def swap(value, count, distance):
    return lax.ppermute(value, AXES, [(i, i ^ distance) for i in range(count)])


def me(n_tp):
    return lax.axis_index("dp") * n_tp + lax.axis_index("tp")


def params(**kwargs):
    return pltpu.CompilerParams(vmem_limit_bytes=16 * 1024 * 1024, **kwargs)


def pack_kernel(n_tp, plane, planes, sub, block, x_ref, s_ref, *outs):
    index = me(n_tp)
    scales = s_ref[...].T
    blocks = scales.shape[1]
    lane = lax.broadcasted_iota(jnp.int32, (blocks, sub), 1) // block
    row = lax.broadcasted_iota(jnp.int32, (blocks, sub), 0)
    for k, out in enumerate(outs):
        for n, j in enumerate(planes):
            part = lax.bitwise_xor(index, jnp.int32(j * plane + k))
            pick = (row == lane + part * (sub // block)).astype(jnp.bfloat16)
            spread = jnp.dot(scales, pick, preferred_element_type=jnp.float32)
            values = x_ref[:, pl.ds(pl.multiple_of(part * sub, sub), sub)].astype(jnp.float32)
            out[:, n * sub:(n + 1) * sub] = (values * spread).astype(jnp.bfloat16)


def pack(x, scales, n_tp, plane, planes, sub):
    rows = x.shape[0]
    block = x.shape[1] // scales.shape[0]
    shape = jax.ShapeDtypeStruct((rows, len(planes) * sub), jnp.bfloat16)
    return pl.pallas_call(
        functools.partial(pack_kernel, n_tp, plane, planes, sub, block),
        out_shape=[shape] * plane,
        in_specs=[VMEM] * 2,
        out_specs=[VMEM] * plane,
        compiler_params=params(),
        cost_estimate=pl.CostEstimate(
            flops=2 * rows * sub * len(planes) * plane,
            bytes_accessed=4 * rows * sub * len(planes) * plane,
            transcendentals=0,
        ),
        name="pack",
    )(x, scales)


def grads_kernel(n_tp, rows, *refs):
    *ins, out = refs
    tp = lax.axis_index("tp")
    hd = ins[0].shape[1]
    for g in range(len(ins) // n_tp):
        for kt in range(n_tp):
            start = pl.multiple_of(lax.bitwise_xor(tp, jnp.int32(kt)) * rows, rows)
            for h in range(n_tp):
                piece = ins[g * n_tp + h][pl.ds(start, rows), :]
                column = (g * n_tp + kt) * rows
                out[h * hd:(h + 1) * hd, column:column + rows] = piece.T


def grads(pieces, n_tp, rows):
    hd = pieces[0].shape[1]
    return pl.pallas_call(
        functools.partial(grads_kernel, n_tp, rows),
        out_shape=jax.ShapeDtypeStruct((n_tp * hd, len(pieces) * rows), jnp.bfloat16),
        in_specs=[VMEM] * len(pieces),
        out_specs=VMEM,
        compiler_params=params(),
        cost_estimate=pl.CostEstimate(
            flops=len(pieces) * rows * hd * n_tp, bytes_accessed=4 * len(pieces) * rows * hd * n_tp, transcendentals=0
        ),
        name="grads",
    )(*pieces)


def matmul_kernel(sub, n_grads, *refs):
    gt = jnp.concatenate([r[...] for r in refs[:n_grads]], axis=1)
    outs = [r for r in refs if r.shape[0] == gt.shape[0]][n_grads:]
    ins = refs[n_grads:len(refs) - len(outs)]
    x = jnp.concatenate([r[...] for r in ins], axis=0)
    for n, out in enumerate(outs):
        total = jnp.dot(gt, x[:, n * sub:(n + 1) * sub], preferred_element_type=jnp.float32)
        out[...] = total.astype(out.dtype)


def matmul(gts, xs, types, sub):
    columns = gts[0].shape[0]
    tokens = sum(x.shape[0] for x in xs)
    return pl.pallas_call(
        functools.partial(matmul_kernel, sub, len(gts)),
        out_shape=[jax.ShapeDtypeStruct((columns, sub), t) for t in types],
        in_specs=[VMEM] * (len(gts) + len(xs)),
        out_specs=[VMEM] * len(types),
        compiler_params=params(),
        cost_estimate=pl.CostEstimate(
            flops=2 * columns * tokens * sub * len(types),
            bytes_accessed=2 * tokens * sub * len(types),
            transcendentals=0,
        ),
        name="matmul",
    )(*gts, *xs)


def total_kernel(*refs):
    *ins, own, other, squares = refs
    total = ins[0][...]
    for r in ins[1:]:
        total = total + r[...].astype(jnp.float32)
    half = own.shape[0]
    own[...] = total[:half]
    other[...] = total[half:]
    squared = total * total
    squares[...] = squared.reshape(-1, 8, squared.shape[1]).sum(0)[:, :128] + sum(
        squared.reshape(-1, 8, squared.shape[1]).sum(0)[:, n:n + 128] for n in range(128, squared.shape[1], 128)
    )


def totals(parts):
    columns, sub = parts[0].shape
    half = jax.ShapeDtypeStruct((columns // 2, sub), jnp.float32)
    return pl.pallas_call(
        total_kernel,
        out_shape=[half, half, jax.ShapeDtypeStruct((8, 128), jnp.float32)],
        in_specs=[VMEM] * len(parts),
        out_specs=[VMEM] * 3,
        compiler_params=params(),
        cost_estimate=pl.CostEstimate(flops=8 * columns * sub, bytes_accessed=8 * columns * sub, transcendentals=0),
        name="totals",
    )(*parts)


def clip_kernel(limit_squared, own, other, *refs):
    *squares, out = refs
    tp = lax.axis_index("tp")
    sub = own.shape[1]
    total = jnp.sum(sum(r[...] for r in squares))
    norm = jnp.sqrt(jnp.full((8, 128), total, jnp.float32))
    factor = jnp.minimum(jnp.float32(1.0), jnp.sqrt(jnp.float32(limit_squared)) / norm)[:1]
    out[pl.ds(pl.multiple_of(tp * sub, sub), sub), :] = own[...].T * factor
    out[pl.ds(pl.multiple_of((1 - tp) * sub, sub), sub), :] = other[...].T * factor


def clip(own, other, squares, limit_squared):
    hd, sub = own.shape
    return pl.pallas_call(
        functools.partial(clip_kernel, limit_squared),
        out_shape=jax.ShapeDtypeStruct((2 * sub, hd), jnp.float32),
        in_specs=[VMEM] * (2 + len(squares)),
        out_specs=VMEM,
        compiler_params=params(),
        cost_estimate=pl.CostEstimate(flops=4 * hd * sub, bytes_accessed=16 * hd * sub, transcendentals=0),
        name="clip",
    )(own, other, *squares)


def fast_body(inner, stash_values, stash_scales, value_grad):
    n_dp, n_tp = lax.axis_size("dp"), lax.axis_size("tp")
    count = n_dp * n_tp
    plane = inner * n_tp
    depth = count // plane
    rows, width = stash_values.shape
    sub = width // count
    send = functools.partial(swap, count=count)

    chunks = [tuple(range(depth - 1, 1, -1)), (1, 0)]
    scales = stash_scales.T

    far = inner // 2 * n_tp
    near = [value_grad] + [send(value_grad, distance=k) for k in range(1, n_tp)]
    near += [send(value_grad, distance=far + k) for k in range(n_tp)]
    gts = [grads(near, n_tp, rows)]
    order = list(range(n_tp)) + [far + k for k in range(n_tp)]
    orders = list(order)
    step = n_tp
    while step < far:
        gts += [send(g, distance=step) for g in gts]
        orders += [k ^ step for k in orders]
        step *= 2

    parts = []
    for planes in chunks:
        packed = pack(stash_values, scales, n_tp, plane, planes, sub)
        arrived = [packed[0]]
        for k in range(1, plane):
            arrived.append(send(packed[k], distance=k))
        types = [jnp.bfloat16 if j else jnp.float32 for j in planes]
        products = matmul(gts, [arrived[k] for k in orders], types, sub)
        parts += [send(q, distance=j * plane) if j else q for j, q in zip(planes, products)]
    own, other, squares = totals(parts[::-1])
    other = send(other, distance=1)

    groups = [(n_tp,), (1, far, far + 1), tuple(j * plane for j in range(1, depth))]
    pieces = [squares]
    for group in groups:
        merged = sum(pieces[1:], pieces[0])
        pieces = [merged] + [send(merged, distance=k) for k in group]
    columns = value_grad.shape[1] * n_tp
    return clip(own, other, pieces, width * columns)


def block_dequantize(values, scales):
    rows = values.shape[0]
    blocks = scales.shape[1]
    scaled = (
        values.astype(jnp.float32).reshape(rows, blocks, values.shape[1] // blocks)
        * scales.astype(jnp.float32)[:, :, None]
    )
    return scaled.reshape(rows, values.shape[1]).astype(jnp.bfloat16)


def body(stash_values, stash_scales, value_grad):
    width = stash_values.shape[1]
    columns = value_grad.shape[1]
    dp_count = lax.axis_size("dp")
    tp_count = lax.axis_size("tp")
    own_tokens = stash_values.shape[0]
    sub_rows = width // (dp_count * tp_count)
    if tp_count == 2 and dp_count == 16 and sub_rows % 256 == 0 and own_tokens % 128 == 0 and columns == 128:
        return fast_body(4, stash_values, stash_scales, value_grad)
    inputs = block_dequantize(stash_values, stash_scales)
    inputs = inputs.reshape(own_tokens, dp_count, tp_count, sub_rows)
    features = lax.all_to_all(inputs, "tp", split_axis=2, concat_axis=0, tiled=True)
    features = features.reshape(own_tokens * tp_count, dp_count * sub_rows)
    all_heads = lax.dot_general(
        features,
        lax.all_gather(value_grad, "tp", axis=1, tiled=True),
        (((0,), (0,)), ((), ())),
        preferred_element_type=jnp.float32,
    )
    summed = lax.psum_scatter(all_heads, "dp", scatter_dimension=0, tiled=True)
    local = lax.all_to_all(summed, "tp", split_axis=1, concat_axis=0, tiled=True)
    total = lax.psum(jnp.sum(summed * summed), ("dp", "tp"))
    limit = jnp.sqrt(jnp.float32(width * columns * lax.axis_size("tp")))
    return local * jnp.minimum(jnp.float32(1.0), limit / jnp.sqrt(total))


def solution(mesh):
    placed = (P(("dp", "tp"), None), P(("dp", "tp"), None), P("dp", "tp"))
    return jax.shard_map(body, mesh=mesh, in_specs=placed, out_specs=P("dp", "tp"), check_vma=False)
```

```python
import functools

import jax
import jax.numpy as jnp
from jax import lax
from jax.experimental import pallas as pl
from jax.experimental.pallas import tpu as pltpu
from jax.sharding import PartitionSpec as P


AXES = ("dp", "tp")
VMEM = pl.BlockSpec(memory_space=pltpu.VMEM)


def params(limit=16 * 1024 * 1024):
    return pltpu.CompilerParams(vmem_limit_bytes=limit)


def cost(flops, moved):
    return pl.CostEstimate(flops=flops, bytes_accessed=moved, transcendentals=0)


def dequantize(values, scales, first, sub, block):
    blocks = scales.shape[0]
    row = lax.broadcasted_iota(jnp.int32, (blocks, sub), 0)
    lane = lax.broadcasted_iota(jnp.int32, (blocks, sub), 1) // block
    pick = (row == lane + first).astype(jnp.bfloat16)
    spread = lax.dot_general(scales, pick, (((0,), (0,)), ((), ())), preferred_element_type=jnp.float32)
    return (values.astype(jnp.float32) * spread).astype(jnp.bfloat16)


def pack_kernel(n_tp, plane, planes, keys, core, sub, block, load, x_ref, s_ref, *refs):
    index = lax.axis_index("dp") * n_tp + lax.axis_index("tp")
    base = 0
    if load:
        *outs, x_vmem, s_vmem, sems = refs
        (j,) = planes
        width = plane * sub
        base = lax.bitwise_xor(index, jnp.int32(j * plane)) // plane * plane
        copies = [
            pltpu.make_async_copy(
                x_ref.at[:, pl.ds(pl.multiple_of(base * sub, width), width)], x_vmem, sems.at[0]
            ),
            pltpu.make_async_copy(s_ref, s_vmem, sems.at[1]),
        ]
        for copy in copies:
            copy.start()
        for copy in copies:
            copy.wait()
        x_ref, s_ref = x_vmem, s_vmem
    else:
        outs = refs
    scales = s_ref[...]
    for n, j in enumerate(planes):
        for m, key in enumerate(keys):
            out = outs[n * len(keys) + m]
            for h in range(2):
                part = lax.bitwise_xor(index, jnp.int32((j * plane + key) ^ (h * core)))
                values = x_ref[:, pl.ds(pl.multiple_of((part - base) * sub, sub), sub)]
                out[:, h * sub:(h + 1) * sub] = dequantize(values, scales, part * (sub // block), sub, block)


def pack(x, scales, n_tp, plane, planes, keys, core, sub, load):
    rows = x.shape[0]
    block = x.shape[1] // scales.shape[0]
    outs = len(planes) * len(keys)
    scratch = [
        pltpu.VMEM((rows, plane * sub), x.dtype),
        pltpu.VMEM(scales.shape, scales.dtype),
        pltpu.SemaphoreType.DMA((2,)),
    ]
    return pl.pallas_call(
        functools.partial(pack_kernel, n_tp, plane, planes, keys, core, sub, block, load),
        out_shape=[jax.ShapeDtypeStruct((rows, 2 * sub), jnp.bfloat16)] * outs,
        in_specs=[pl.BlockSpec(memory_space=pltpu.HBM)] * 2 if load else [VMEM] * 2,
        out_specs=[VMEM] * outs,
        scratch_shapes=scratch if load else [],
        compiler_params=params(67_043_328 - x.size * 5 // 4) if load else params(),
        cost_estimate=cost(4 * rows * sub * outs, 8 * rows * sub * outs),
        name="pack",
    )(x, scales)


def grads_kernel(n_tp, rows, *refs):
    *ins, out = refs
    tp = lax.axis_index("tp")
    hd = ins[0].shape[1]
    for g in range(len(ins) // n_tp):
        for kt in range(n_tp):
            start = pl.multiple_of(lax.bitwise_xor(tp, jnp.int32(kt)) * rows, rows)
            for h in range(n_tp):
                piece = ins[g * n_tp + h][pl.ds(start, rows), :]
                column = (g * n_tp + kt) * rows
                out[h * hd:(h + 1) * hd, column:column + rows] = piece.T


def grads(pieces, n_tp, rows):
    hd = pieces[0].shape[1]
    size = len(pieces) * rows * hd * n_tp
    return pl.pallas_call(
        functools.partial(grads_kernel, n_tp, rows),
        out_shape=jax.ShapeDtypeStruct((n_tp * hd, len(pieces) * rows), jnp.bfloat16),
        in_specs=[VMEM] * len(pieces),
        out_specs=VMEM,
        compiler_params=params(),
        cost_estimate=cost(size, 4 * size),
        name="grads",
    )(*pieces)


def matmul_kernel(sub, gt_ref, *refs):
    *ins, mine, theirs = refs
    gt = gt_ref[...]
    x = jnp.concatenate([r[...] for r in ins], axis=0)
    theirs[...] = jnp.dot(gt, x[:, sub:], preferred_element_type=jnp.float32)
    mine[...] = jnp.dot(gt, x[:, :sub], preferred_element_type=jnp.float32)


def matmul(gt, xs, sub):
    columns, tokens = gt.shape
    return pl.pallas_call(
        functools.partial(matmul_kernel, sub),
        out_shape=[jax.ShapeDtypeStruct((columns, sub), jnp.float32)] * 2,
        in_specs=[VMEM] * (1 + len(xs)),
        out_specs=[VMEM] * 2,
        compiler_params=params(),
        cost_estimate=cost(4 * columns * tokens * sub, 4 * tokens * sub),
        name="matmul",
    )(gt, *xs)


def join_kernel(a, b, out):
    out[...] = (a[...] + b[...]).astype(out.dtype)


def join(a, b):
    return pl.pallas_call(
        join_kernel,
        out_shape=jax.ShapeDtypeStruct(a.shape, jnp.bfloat16),
        in_specs=[VMEM] * 2,
        out_specs=VMEM,
        compiler_params=params(),
        cost_estimate=cost(a.size, 10 * a.size),
        name="join",
    )(a, b)


def total_kernel(*refs):
    *ins, own, other, squares = refs
    total = ins[0][...]
    for r in ins[1:]:
        total = total + r[...].astype(jnp.float32)
    half = own.shape[0]
    own[...] = total[:half]
    other[...] = total[half:]
    squared = (total * total).reshape(-1, 8, total.shape[1]).sum(0)
    squares[...] = sum(squared[:, n:n + 128] for n in range(128, squared.shape[1], 128)) + squared[:, :128]


def totals(parts):
    columns, sub = parts[0].shape
    half = jax.ShapeDtypeStruct((columns // 2, sub), jnp.float32)
    return pl.pallas_call(
        total_kernel,
        out_shape=[half, half, jax.ShapeDtypeStruct((8, 128), jnp.float32)],
        in_specs=[VMEM] * len(parts),
        out_specs=[VMEM] * 3,
        compiler_params=params(),
        cost_estimate=cost(8 * columns * sub, 8 * columns * sub),
        name="totals",
    )(*parts)


def clip_kernel(limit_squared, own, other, *refs):
    *squares, out = refs
    tp = lax.axis_index("tp")
    sub = own.shape[1]
    total = jnp.sum(sum(r[...] for r in squares))
    norm = jnp.sqrt(jnp.full((8, 128), total, jnp.float32))
    factor = jnp.minimum(jnp.float32(1.0), jnp.sqrt(jnp.float32(limit_squared)) / norm)[:1]
    out[pl.ds(pl.multiple_of(tp * sub, sub), sub), :] = own[...].T * factor
    out[pl.ds(pl.multiple_of((1 - tp) * sub, sub), sub), :] = other[...].T * factor


def clip(own, other, squares, limit_squared):
    hd, sub = own.shape
    return pl.pallas_call(
        functools.partial(clip_kernel, limit_squared),
        out_shape=jax.ShapeDtypeStruct((2 * sub, hd), jnp.float32),
        in_specs=[VMEM] * (2 + len(squares)),
        out_specs=VMEM,
        compiler_params=params(),
        cost_estimate=cost(4 * hd * sub, 16 * hd * sub),
        name="clip",
    )(own, other, *squares)


INNER = 4


def keys_of(n_tp):
    far = INNER // 2 * n_tp
    return [0] + list(range(1, n_tp)) + [far + k for k in range(n_tp)]


def fast_body(stash_values, stash_scales, value_grad):
    n_dp, n_tp = lax.axis_size("dp"), lax.axis_size("tp")
    count = n_dp * n_tp
    plane = INNER * n_tp
    depth = count // plane
    rows, width = stash_values.shape
    sub = width // count
    keys = keys_of(n_tp)
    core = n_tp
    scales = stash_scales.T

    def send(value, distance):
        return lax.ppermute(value, AXES, [(i, i ^ distance) for i in range(count)])

    order = list(range(depth - 1, -1, -1))
    packed = pack(stash_values, scales, n_tp, plane, order[:1], keys, core, sub, True)
    packed += pack(stash_values, scales, n_tp, plane, order[1:], keys, core, sub, False)
    near = [value_grad] + [send(value_grad, k) for k in keys[1:]]
    gt = grads(near, n_tp, rows)
    parts = []
    for n, j in enumerate(order):
        own, *away = packed[n * len(keys):(n + 1) * len(keys)]
        arrived = [own] + [send(v, k) for k, v in zip(keys[1:], away)]
        mine, theirs = matmul(gt, arrived, sub)
        theirs = send(theirs, core)
        if j:
            parts.append(send(join(mine, theirs), j * plane))
        else:
            parts += [mine, theirs]
    own, other, squares = totals(parts[::-1])
    other = send(other, 1)

    pieces = [squares]
    for group in [(core,), keys[1:], [j * plane for j in range(1, depth)]]:
        merged = sum(pieces[1:], pieces[0])
        pieces = [merged] + [send(merged, k) for k in group]
    columns = value_grad.shape[1] * n_tp
    return clip(own, other, pieces, width * columns)


def block_dequantize(values, scales):
    rows = values.shape[0]
    blocks = scales.shape[1]
    scaled = (
        values.astype(jnp.float32).reshape(rows, blocks, values.shape[1] // blocks)
        * scales.astype(jnp.float32)[:, :, None]
    )
    return scaled.reshape(rows, values.shape[1]).astype(jnp.bfloat16)


def body(stash_values, stash_scales, value_grad):
    width = stash_values.shape[1]
    columns = value_grad.shape[1]
    dp_count = lax.axis_size("dp")
    tp_count = lax.axis_size("tp")
    own_tokens = stash_values.shape[0]
    sub_rows = width // (dp_count * tp_count)
    if tp_count == 2 and dp_count == 16 and sub_rows % 256 == 0 and own_tokens % 128 == 0 and columns == 128:
        return fast_body(stash_values, stash_scales, value_grad)
    inputs = block_dequantize(stash_values, stash_scales)
    inputs = inputs.reshape(own_tokens, dp_count, tp_count, sub_rows)
    features = lax.all_to_all(inputs, "tp", split_axis=2, concat_axis=0, tiled=True)
    features = features.reshape(own_tokens * tp_count, dp_count * sub_rows)
    all_heads = lax.dot_general(
        features,
        lax.all_gather(value_grad, "tp", axis=1, tiled=True),
        (((0,), (0,)), ((), ())),
        preferred_element_type=jnp.float32,
    )
    summed = lax.psum_scatter(all_heads, "dp", scatter_dimension=0, tiled=True)
    local = lax.all_to_all(summed, "tp", split_axis=1, concat_axis=0, tiled=True)
    total = lax.psum(jnp.sum(summed * summed), ("dp", "tp"))
    limit = jnp.sqrt(jnp.float32(width * columns * lax.axis_size("tp")))
    return local * jnp.minimum(jnp.float32(1.0), limit / jnp.sqrt(total))


def solution(mesh):
    placed = (P(("dp", "tp"), None), P(("dp", "tp"), None), P("dp", "tp"))
    return jax.shard_map(body, mesh=mesh, in_specs=placed, out_specs=P("dp", "tp"), check_vma=False)
```

```python
import functools

import jax
import jax.numpy as jnp
from jax import lax
from jax.experimental import pallas as pl
from jax.experimental.pallas import tpu as pltpu
from jax.sharding import PartitionSpec as P


AXES = ("dp", "tp")
VMEM = pl.BlockSpec(memory_space=pltpu.VMEM)


def params(limit=16 * 1024 * 1024):
    return pltpu.CompilerParams(vmem_limit_bytes=limit)


def cost(flops, moved):
    return pl.CostEstimate(flops=flops, bytes_accessed=moved, transcendentals=0)


def dequantize(values, scales, first, sub, block):
    blocks = scales.shape[0]
    row = lax.broadcasted_iota(jnp.int32, (blocks, sub), 0)
    lane = lax.broadcasted_iota(jnp.int32, (blocks, sub), 1) // block
    pick = (row == lane + first).astype(jnp.bfloat16)
    spread = lax.dot_general(scales, pick, (((0,), (0,)), ((), ())), preferred_element_type=jnp.float32)
    return (values.astype(jnp.float32) * spread).astype(jnp.bfloat16)


def pack_kernel(n_tp, plane, planes, keys, core, sub, block, load, x_ref, s_ref, *refs):
    index = lax.axis_index("dp") * n_tp + lax.axis_index("tp")
    base = 0
    if load:
        g_ref, *outs, x_vmem, s_vmem, sems = refs
        (j,) = planes
        width = plane * sub
        base = lax.bitwise_xor(index, jnp.int32(j * plane)) // plane * plane
        copies = [
            pltpu.make_async_copy(
                x_ref.at[:, pl.ds(pl.multiple_of(base * sub, width), width)], x_vmem, sems.at[0]
            ),
            pltpu.make_async_copy(s_ref, s_vmem, sems.at[1]),
        ]
        for copy in copies:
            copy.start()
        for copy in copies:
            copy.wait()
        x_ref, s_ref = x_vmem, s_vmem
        rows = x_vmem.shape[0]
        for out in outs:
            for h in range(n_tp):
                hd = g_ref.shape[1]
                out[:, 2 * sub + h * hd:2 * sub + (h + 1) * hd] = g_ref[h * rows:(h + 1) * rows, :]
    else:
        outs = refs
    scales = s_ref[...]
    for n, j in enumerate(planes):
        for m, key in enumerate(keys):
            out = outs[n * len(keys) + m]
            for h in range(2):
                part = lax.bitwise_xor(index, jnp.int32((j * plane + key) ^ (h * core)))
                values = x_ref[:, pl.ds(pl.multiple_of((part - base) * sub, sub), sub)]
                out[:, h * sub:(h + 1) * sub] = dequantize(values, scales, part * (sub // block), sub, block)


def pack(x, scales, n_tp, plane, planes, keys, core, sub, *load):
    rows = x.shape[0]
    extra = load[0].size // rows if load else 0
    block = x.shape[1] // scales.shape[0]
    outs = len(planes) * len(keys)
    scratch = [
        pltpu.VMEM((rows, plane * sub), x.dtype),
        pltpu.VMEM(scales.shape, scales.dtype),
        pltpu.SemaphoreType.DMA((2,)),
    ]
    return pl.pallas_call(
        functools.partial(pack_kernel, n_tp, plane, planes, keys, core, sub, block, bool(load)),
        out_shape=[jax.ShapeDtypeStruct((rows, 2 * sub + extra), jnp.bfloat16)] * outs,
        in_specs=[pl.BlockSpec(memory_space=pltpu.HBM)] * 2 + [VMEM] if load else [VMEM] * 2,
        out_specs=[VMEM] * outs,
        scratch_shapes=scratch if load else [],
        compiler_params=params(FIRST_LIMIT) if load else params(),
        cost_estimate=cost(4 * rows * sub * outs, 8 * rows * sub * outs),
        name="pack",
    )(x, scales, *load)


def grads_kernel(n_tp, rows, hd, base, *refs):
    *ins, out = refs
    tp = lax.axis_index("tp")
    for g in range(len(ins) // n_tp):
        for kt in range(n_tp):
            start = pl.multiple_of(base + lax.bitwise_xor(tp, jnp.int32(kt)) * hd, hd)
            for h in range(n_tp):
                piece = ins[g * n_tp + h][:, pl.ds(start, hd)]
                column = (g * n_tp + kt) * rows
                out[h * hd:(h + 1) * hd, column:column + rows] = piece.T


def grads(pieces, n_tp, hd, base):
    rows = pieces[0].shape[0]
    size = len(pieces) * rows * hd * n_tp
    return pl.pallas_call(
        functools.partial(grads_kernel, n_tp, rows, hd, base),
        out_shape=jax.ShapeDtypeStruct((n_tp * hd, len(pieces) * rows), jnp.bfloat16),
        in_specs=[VMEM] * len(pieces),
        out_specs=VMEM,
        compiler_params=params(),
        cost_estimate=cost(size, 4 * size),
        name="grads",
    )(*pieces)


def matmul_kernel(sub, gt_ref, *refs):
    *ins, mine, theirs = refs
    gt = gt_ref[...]
    x = jnp.concatenate([r[:, :2 * sub] for r in ins], axis=0)
    theirs[...] = jnp.dot(gt, x[:, sub:], preferred_element_type=jnp.float32)
    mine[...] = jnp.dot(gt, x[:, :sub], preferred_element_type=jnp.float32)


def matmul(gt, xs, sub):
    columns, tokens = gt.shape
    return pl.pallas_call(
        functools.partial(matmul_kernel, sub),
        out_shape=[jax.ShapeDtypeStruct((columns, sub), jnp.float32)] * 2,
        in_specs=[VMEM] * (1 + len(xs)),
        out_specs=[VMEM] * 2,
        compiler_params=params(),
        cost_estimate=cost(4 * columns * tokens * sub, 4 * tokens * sub),
        name="matmul",
    )(gt, *xs)


def join_kernel(a, b, out):
    out[...] = (a[...] + b[...]).astype(out.dtype)


def join(a, b):
    return pl.pallas_call(
        join_kernel,
        out_shape=jax.ShapeDtypeStruct(a.shape, jnp.bfloat16),
        in_specs=[VMEM] * 2,
        out_specs=VMEM,
        compiler_params=params(),
        cost_estimate=cost(a.size, 10 * a.size),
        name="join",
    )(a, b)


def total_kernel(*refs):
    *ins, own, other, squares = refs
    total = ins[0][...]
    for r in ins[1:]:
        total = total + r[...].astype(jnp.float32)
    half = own.shape[0]
    own[...] = total[:half]
    other[...] = total[half:]
    squared = (total * total).reshape(-1, 8, total.shape[1]).sum(0)
    squares[...] = sum(squared[:, n:n + 128] for n in range(128, squared.shape[1], 128)) + squared[:, :128]


def totals(parts):
    columns, sub = parts[0].shape
    half = jax.ShapeDtypeStruct((columns // 2, sub), jnp.float32)
    return pl.pallas_call(
        total_kernel,
        out_shape=[half, half, jax.ShapeDtypeStruct((8, 128), jnp.float32)],
        in_specs=[VMEM] * len(parts),
        out_specs=[VMEM] * 3,
        compiler_params=params(),
        cost_estimate=cost(8 * columns * sub, 8 * columns * sub),
        name="totals",
    )(*parts)


def clip_kernel(limit_squared, own, other, *refs):
    *squares, out = refs
    tp = lax.axis_index("tp")
    sub = own.shape[1]
    total = jnp.sum(sum(r[...] for r in squares))
    norm = jnp.sqrt(jnp.full((8, 128), total, jnp.float32))
    factor = jnp.minimum(jnp.float32(1.0), jnp.sqrt(jnp.float32(limit_squared)) / norm)[:1]
    out[pl.ds(pl.multiple_of(tp * sub, sub), sub), :] = own[...].T * factor
    out[pl.ds(pl.multiple_of((1 - tp) * sub, sub), sub), :] = other[...].T * factor


def clip(own, other, squares, limit_squared):
    hd, sub = own.shape
    return pl.pallas_call(
        functools.partial(clip_kernel, limit_squared),
        out_shape=jax.ShapeDtypeStruct((2 * sub, hd), jnp.float32),
        in_specs=[VMEM] * (2 + len(squares)),
        out_specs=VMEM,
        compiler_params=params(),
        cost_estimate=cost(4 * hd * sub, 16 * hd * sub),
        name="clip",
    )(own, other, *squares)


FIRST_LIMIT = 54_000_000
INNER = 4


def keys_of(n_tp):
    far = INNER // 2 * n_tp
    return [0] + list(range(1, n_tp)) + [far + k for k in range(n_tp)]


def fast_body(stash_values, stash_scales, value_grad):
    n_dp, n_tp = lax.axis_size("dp"), lax.axis_size("tp")
    count = n_dp * n_tp
    plane = INNER * n_tp
    depth = count // plane
    _, width = stash_values.shape
    sub = width // count
    keys = keys_of(n_tp)
    core = n_tp
    scales = stash_scales.T

    def send(value, distance):
        return lax.ppermute(value, AXES, [(i, i ^ distance) for i in range(count)])

    order = list(range(depth - 1, -1, -1))
    packed = pack(stash_values, scales, n_tp, plane, order[:1], keys, core, sub, value_grad)
    packed += pack(stash_values, scales, n_tp, plane, order[1:], keys, core, sub)
    parts = []
    for n, j in enumerate(order):
        own, *away = packed[n * len(keys):(n + 1) * len(keys)]
        arrived = [own] + [send(v, k) for k, v in zip(keys[1:], away)]
        if n == 0:
            gt = grads(arrived, n_tp, value_grad.shape[1], 2 * sub)
        mine, theirs = matmul(gt, arrived, sub)
        theirs = send(theirs, core)
        if j:
            parts.append(send(join(mine, theirs), j * plane))
        else:
            parts += [mine, theirs]
    own, other, squares = totals(parts[::-1])
    other = send(other, 1)

    pieces = [squares]
    for group in [(core,), keys[1:], [j * plane for j in range(1, depth)]]:
        merged = sum(pieces[1:], pieces[0])
        pieces = [merged] + [send(merged, k) for k in group]
    columns = value_grad.shape[1] * n_tp
    return clip(own, other, pieces, width * columns)


def block_dequantize(values, scales):
    rows = values.shape[0]
    blocks = scales.shape[1]
    scaled = (
        values.astype(jnp.float32).reshape(rows, blocks, values.shape[1] // blocks)
        * scales.astype(jnp.float32)[:, :, None]
    )
    return scaled.reshape(rows, values.shape[1]).astype(jnp.bfloat16)


def body(stash_values, stash_scales, value_grad):
    width = stash_values.shape[1]
    columns = value_grad.shape[1]
    dp_count = lax.axis_size("dp")
    tp_count = lax.axis_size("tp")
    own_tokens = stash_values.shape[0]
    sub_rows = width // (dp_count * tp_count)
    if tp_count == 2 and dp_count == 16 and sub_rows % 256 == 0 and own_tokens % 128 == 0 and columns == 128:
        return fast_body(stash_values, stash_scales, value_grad)
    inputs = block_dequantize(stash_values, stash_scales)
    inputs = inputs.reshape(own_tokens, dp_count, tp_count, sub_rows)
    features = lax.all_to_all(inputs, "tp", split_axis=2, concat_axis=0, tiled=True)
    features = features.reshape(own_tokens * tp_count, dp_count * sub_rows)
    all_heads = lax.dot_general(
        features,
        lax.all_gather(value_grad, "tp", axis=1, tiled=True),
        (((0,), (0,)), ((), ())),
        preferred_element_type=jnp.float32,
    )
    summed = lax.psum_scatter(all_heads, "dp", scatter_dimension=0, tiled=True)
    local = lax.all_to_all(summed, "tp", split_axis=1, concat_axis=0, tiled=True)
    total = lax.psum(jnp.sum(summed * summed), ("dp", "tp"))
    limit = jnp.sqrt(jnp.float32(width * columns * lax.axis_size("tp")))
    return local * jnp.minimum(jnp.float32(1.0), limit / jnp.sqrt(total))


def solution(mesh):
    placed = (P(("dp", "tp"), None), P(("dp", "tp"), None), P("dp", "tp"))
    return jax.shard_map(body, mesh=mesh, in_specs=placed, out_specs=P("dp", "tp"), check_vma=False)
```

```python
import functools

import jax
import jax.numpy as jnp
from jax import lax
from jax.experimental import pallas as pl
from jax.experimental.pallas import tpu as pltpu
from jax.sharding import PartitionSpec as P


AXES = ("dp", "tp")
VMEM = pl.BlockSpec(memory_space=pltpu.VMEM)


def params(limit=16 * 1024 * 1024):
    return pltpu.CompilerParams(vmem_limit_bytes=limit)


def cost(flops, moved):
    return pl.CostEstimate(flops=flops, bytes_accessed=moved, transcendentals=0)


def dequantize(values, scales, first, sub, block):
    blocks = scales.shape[0]
    row = lax.broadcasted_iota(jnp.int32, (blocks, sub), 0)
    lane = lax.broadcasted_iota(jnp.int32, (blocks, sub), 1) // block
    pick = (row == lane + first).astype(jnp.bfloat16)
    spread = lax.dot_general(scales, pick, (((0,), (0,)), ((), ())), preferred_element_type=jnp.float32)
    return (values.astype(jnp.float32) * spread).astype(jnp.bfloat16)


def pack_kernel(n_tp, plane, planes, keys, core, sub, block, load, x_ref, s_ref, *refs):
    index = lax.axis_index("dp") * n_tp + lax.axis_index("tp")
    base = 0
    if load:
        *outs, x_vmem, sem = refs
        (j,) = planes
        width = plane * sub
        base = lax.bitwise_xor(index, jnp.int32(j * plane)) // plane * plane
        copy = pltpu.make_async_copy(
            x_ref.at[:, pl.ds(pl.multiple_of(base * sub, width), width)], x_vmem, sem
        )
        copy.start()
        rows = x_vmem.shape[0]
        blocks = s_ref.shape[0] - n_tp * rows
        for out in outs:
            for h in range(n_tp):
                hd = s_ref.shape[1]
                out[:, 2 * sub + h * hd:2 * sub + (h + 1) * hd] = s_ref[blocks + h * rows:blocks + (h + 1) * rows, :]
        copy.wait()
        x_ref, s_ref = x_vmem, s_ref.at[:blocks]
    else:
        outs = refs
    scales = s_ref[...]
    for n, j in enumerate(planes):
        for m, key in enumerate(keys):
            out = outs[n * len(keys) + m]
            for h in range(2):
                part = lax.bitwise_xor(index, jnp.int32((j * plane + key) ^ (h * core)))
                values = x_ref[:, pl.ds(pl.multiple_of((part - base) * sub, sub), sub)]
                out[:, h * sub:(h + 1) * sub] = dequantize(values, scales, part * (sub // block), sub, block)


def pack(x, scales, n_tp, plane, planes, keys, core, sub, *load):
    rows = x.shape[0]
    extra = load[0].size // rows if load else 0
    block = x.shape[1] // (scales.shape[0] - (load[0].shape[0] if load else 0))
    outs = len(planes) * len(keys)
    scratch = [
        pltpu.VMEM((rows, plane * sub), x.dtype),
        pltpu.SemaphoreType.DMA,
    ]
    return pl.pallas_call(
        functools.partial(pack_kernel, n_tp, plane, planes, keys, core, sub, block, bool(load)),
        out_shape=[jax.ShapeDtypeStruct((rows, 2 * sub + extra), jnp.bfloat16)] * outs,
        in_specs=[pl.BlockSpec(memory_space=pltpu.HBM) if load else VMEM, VMEM],
        out_specs=[VMEM] * outs,
        scratch_shapes=scratch if load else [],
        compiler_params=params(FIRST_LIMIT) if load else params(),
        cost_estimate=cost(4 * rows * sub * outs, 8 * rows * sub * outs),
        name="pack",
    )(x, scales)


def grads_kernel(n_tp, rows, hd, base, *refs):
    *ins, out = refs
    tp = lax.axis_index("tp")
    for g in range(len(ins) // n_tp):
        for kt in range(n_tp):
            start = pl.multiple_of(base + lax.bitwise_xor(tp, jnp.int32(kt)) * hd, hd)
            for h in range(n_tp):
                piece = ins[g * n_tp + h][:, pl.ds(start, hd)]
                column = (g * n_tp + kt) * rows
                out[h * hd:(h + 1) * hd, column:column + rows] = piece.T


def grads(pieces, n_tp, hd, base):
    rows = pieces[0].shape[0]
    size = len(pieces) * rows * hd * n_tp
    return pl.pallas_call(
        functools.partial(grads_kernel, n_tp, rows, hd, base),
        out_shape=jax.ShapeDtypeStruct((n_tp * hd, len(pieces) * rows), jnp.bfloat16),
        in_specs=[VMEM] * len(pieces),
        out_specs=VMEM,
        compiler_params=params(),
        cost_estimate=cost(size, 4 * size),
        name="grads",
    )(*pieces)


def matmul_kernel(sub, gt_ref, *refs):
    *ins, mine, theirs = refs
    gt = gt_ref[...]
    x = jnp.concatenate([r[:, :2 * sub] for r in ins], axis=0)
    theirs[...] = jnp.dot(gt, x[:, sub:], preferred_element_type=jnp.float32)
    mine[...] = jnp.dot(gt, x[:, :sub], preferred_element_type=jnp.float32)


def matmul(gt, xs, sub):
    columns, tokens = gt.shape
    return pl.pallas_call(
        functools.partial(matmul_kernel, sub),
        out_shape=[jax.ShapeDtypeStruct((columns, sub), jnp.float32)] * 2,
        in_specs=[VMEM] * (1 + len(xs)),
        out_specs=[VMEM] * 2,
        compiler_params=params(),
        cost_estimate=cost(4 * columns * tokens * sub, 4 * tokens * sub),
        name="matmul",
    )(gt, *xs)


def join_kernel(*refs):
    *ins, out = refs
    out[...] = sum(r[...].astype(jnp.float32) for r in ins).astype(out.dtype)


def join(*parts):
    a = parts[0]
    return pl.pallas_call(
        join_kernel,
        out_shape=jax.ShapeDtypeStruct(a.shape, jnp.bfloat16),
        in_specs=[VMEM] * len(parts),
        out_specs=VMEM,
        compiler_params=params(),
        cost_estimate=cost(a.size, 10 * a.size),
        name="join",
    )(*parts)


def total_kernel(*refs):
    *ins, own, other, squares = refs
    total = ins[0][...]
    for r in ins[1:]:
        total = total + r[...].astype(jnp.float32)
    half = own.shape[0]
    own[...] = total[:half]
    other[...] = total[half:]
    squared = (total * total).reshape(-1, 8, total.shape[1]).sum(0)
    squares[...] = sum(squared[:, n:n + 128] for n in range(128, squared.shape[1], 128)) + squared[:, :128]


def totals(parts):
    columns, sub = parts[0].shape
    half = jax.ShapeDtypeStruct((columns // 2, sub), jnp.float32)
    return pl.pallas_call(
        total_kernel,
        out_shape=[half, half, jax.ShapeDtypeStruct((8, 128), jnp.float32)],
        in_specs=[VMEM] * len(parts),
        out_specs=[VMEM] * 3,
        compiler_params=params(),
        cost_estimate=cost(8 * columns * sub, 8 * columns * sub),
        name="totals",
    )(*parts)


def clip_kernel(limit_squared, own, other, *refs):
    *squares, out = refs
    tp = lax.axis_index("tp")
    sub = own.shape[1]
    total = jnp.sum(sum(r[...] for r in squares))
    norm = jnp.sqrt(jnp.full((8, 128), total, jnp.float32))
    factor = jnp.minimum(jnp.float32(1.0), jnp.sqrt(jnp.float32(limit_squared)) / norm)[:1]
    out[pl.ds(pl.multiple_of(tp * sub, sub), sub), :] = own[...].T * factor
    out[pl.ds(pl.multiple_of((1 - tp) * sub, sub), sub), :] = other[...].T * factor


def clip(own, other, squares, limit_squared):
    hd, sub = own.shape
    return pl.pallas_call(
        functools.partial(clip_kernel, limit_squared),
        out_shape=jax.ShapeDtypeStruct((2 * sub, hd), jnp.float32),
        in_specs=[VMEM] * (2 + len(squares)),
        out_specs=VMEM,
        compiler_params=params(),
        cost_estimate=cost(4 * hd * sub, 16 * hd * sub),
        name="clip",
    )(own, other, *squares)


FIRST_LIMIT = 54_000_000
INNER = 4


def keys_of(n_tp):
    far = INNER // 2 * n_tp
    return [0] + list(range(1, n_tp)) + [far + k for k in range(n_tp)]


def fast_body(stash_values, stash_scales, value_grad):
    n_dp, n_tp = lax.axis_size("dp"), lax.axis_size("tp")
    count = n_dp * n_tp
    plane = INNER * n_tp
    depth = count // plane
    _, width = stash_values.shape
    sub = width // count
    keys = keys_of(n_tp)
    core = n_tp
    scales = stash_scales.T

    def send(value, distance):
        return lax.ppermute(value, AXES, [(i, i ^ distance) for i in range(count)])

    order = list(range(depth - 1, -1, -1))
    packed = pack(stash_values, jnp.concatenate([scales, value_grad]), n_tp, plane, order[:1], keys, core, sub, value_grad)
    packed += pack(stash_values, scales, n_tp, plane, order[1:], keys, core, sub)
    passed = {}
    for n, j in enumerate(order):
        own, *away = packed[n * len(keys):(n + 1) * len(keys)]
        arrived = [own] + [send(v, k) for k, v in zip(keys[1:], away)]
        if n == 0:
            gt = grads(arrived, n_tp, value_grad.shape[1], 2 * sub)
        mine, theirs = matmul(gt, arrived, sub)
        terms = [mine, send(theirs, core)]
        if j:
            low = j
            terms += passed.pop(j, [])
            value = join(*terms)
            passed.setdefault(j ^ low, []).append(send(value, low * plane))
        else:
            own, other, squares = totals(terms + passed.pop(0))
    other = send(other, 1)
    pieces = [squares]
    for group in [(core,), keys[1:], [j * plane for j in range(1, depth)]]:
        merged = sum(pieces[1:], pieces[0])
        pieces = [merged] + [send(merged, k) for k in group]
    columns = value_grad.shape[1] * n_tp
    return clip(own, other, pieces, width * columns)


def block_dequantize(values, scales):
    rows = values.shape[0]
    blocks = scales.shape[1]
    scaled = (
        values.astype(jnp.float32).reshape(rows, blocks, values.shape[1] // blocks)
        * scales.astype(jnp.float32)[:, :, None]
    )
    return scaled.reshape(rows, values.shape[1]).astype(jnp.bfloat16)


def body(stash_values, stash_scales, value_grad):
    width = stash_values.shape[1]
    columns = value_grad.shape[1]
    dp_count = lax.axis_size("dp")
    tp_count = lax.axis_size("tp")
    own_tokens = stash_values.shape[0]
    sub_rows = width // (dp_count * tp_count)
    if tp_count == 2 and dp_count == 16 and sub_rows % 256 == 0 and own_tokens % 128 == 0 and columns == 128:
        return fast_body(stash_values, stash_scales, value_grad)
    inputs = block_dequantize(stash_values, stash_scales)
    inputs = inputs.reshape(own_tokens, dp_count, tp_count, sub_rows)
    features = lax.all_to_all(inputs, "tp", split_axis=2, concat_axis=0, tiled=True)
    features = features.reshape(own_tokens * tp_count, dp_count * sub_rows)
    all_heads = lax.dot_general(
        features,
        lax.all_gather(value_grad, "tp", axis=1, tiled=True),
        (((0,), (0,)), ((), ())),
        preferred_element_type=jnp.float32,
    )
    summed = lax.psum_scatter(all_heads, "dp", scatter_dimension=0, tiled=True)
    local = lax.all_to_all(summed, "tp", split_axis=1, concat_axis=0, tiled=True)
    total = lax.psum(jnp.sum(summed * summed), ("dp", "tp"))
    limit = jnp.sqrt(jnp.float32(width * columns * lax.axis_size("tp")))
    return local * jnp.minimum(jnp.float32(1.0), limit / jnp.sqrt(total))


def solution(mesh):
    placed = (P(("dp", "tp"), None), P(("dp", "tp"), None), P("dp", "tp"))
    return jax.shard_map(body, mesh=mesh, in_specs=placed, out_specs=P("dp", "tp"), check_vma=False)
```

```python
import functools

import jax
import jax.numpy as jnp
from jax import lax
from jax.experimental import pallas as pl
from jax.experimental.pallas import tpu as pltpu
from jax.sharding import PartitionSpec as P


AXES = ("dp", "tp")
VMEM = pl.BlockSpec(memory_space=pltpu.VMEM)


def params(limit=16 * 1024 * 1024):
    return pltpu.CompilerParams(vmem_limit_bytes=limit)


def cost(flops, moved):
    return pl.CostEstimate(flops=flops, bytes_accessed=moved, transcendentals=0)


def dequantize(values, scales, first, sub, block):
    blocks = scales.shape[0]
    row = lax.broadcasted_iota(jnp.int32, (blocks, sub), 0)
    lane = lax.broadcasted_iota(jnp.int32, (blocks, sub), 1) // block
    pick = (row == lane + first).astype(jnp.bfloat16)
    spread = lax.dot_general(scales, pick, (((0,), (0,)), ((), ())), preferred_element_type=jnp.float32)
    return (values.astype(jnp.float32) * spread).astype(jnp.bfloat16)


def pack_kernel(n_tp, plane, planes, keys, core, sub, block, load, x_ref, s_ref, *refs):
    index = lax.axis_index("dp") * n_tp + lax.axis_index("tp")
    base = 0
    if load:
        *outs, x_vmem, sem = refs
        (j,) = planes
        width = plane * sub
        base = lax.bitwise_xor(index, jnp.int32(j * plane)) // plane * plane
        copy = pltpu.make_async_copy(
            x_ref.at[:, pl.ds(pl.multiple_of(base * sub, width), width)], x_vmem, sem
        )
        copy.start()
        rows = x_vmem.shape[0]
        blocks = s_ref.shape[0] - n_tp * rows
        for out in outs:
            for h in range(n_tp):
                hd = s_ref.shape[1]
                out[:, 2 * sub + h * hd:2 * sub + (h + 1) * hd] = s_ref[blocks + h * rows:blocks + (h + 1) * rows, :]
        copy.wait()
        x_ref, s_ref = x_vmem, s_ref.at[:blocks]
    else:
        outs = refs
    scales = s_ref[...]
    for n, j in enumerate(planes):
        for m, key in enumerate(keys):
            for h in range(2):
                part = lax.bitwise_xor(index, jnp.int32((j * plane + key) ^ (h * core)))
                values = x_ref[:, pl.ds(pl.multiple_of((part - base) * sub, sub), sub)]
                values = dequantize(values, scales, part * (sub // block), sub, block)
                if load:
                    outs[m][:, h * sub:(h + 1) * sub] = values
                else:
                    column = (n * len(keys) + m) * sub
                    outs[h][:, column:column + sub] = values


def pack(x, scales, n_tp, plane, planes, keys, core, sub, *load):
    rows = x.shape[0]
    extra = load[0].size // rows if load else 0
    block = x.shape[1] // (scales.shape[0] - (load[0].shape[0] if load else 0))
    outs = len(keys) if load else 2
    width = 2 * sub + extra if load else len(planes) * len(keys) * sub
    scratch = [
        pltpu.VMEM((rows, plane * sub), x.dtype),
        pltpu.SemaphoreType.DMA,
    ]
    return pl.pallas_call(
        functools.partial(pack_kernel, n_tp, plane, planes, keys, core, sub, block, bool(load)),
        out_shape=[jax.ShapeDtypeStruct((rows, width), jnp.bfloat16)] * outs,
        in_specs=[pl.BlockSpec(memory_space=pltpu.HBM) if load else VMEM, VMEM],
        out_specs=[VMEM] * outs,
        scratch_shapes=scratch if load else [],
        compiler_params=params(FIRST_LIMIT) if load else params(),
        cost_estimate=cost(2 * rows * width * outs, 4 * rows * width * outs),
        name="pack",
    )(x, scales)


def merge_kernel(own, theirs, *outs):
    rows = own.shape[0]
    sub = outs[0].shape[1]
    for n, out in enumerate(outs):
        out[:rows, :] = own[:, n * sub:(n + 1) * sub]
        out[rows:, :] = theirs[:, n * sub:(n + 1) * sub]


def merge(own, theirs, sub):
    rows, width = own.shape
    return pl.pallas_call(
        merge_kernel,
        out_shape=[jax.ShapeDtypeStruct((2 * rows, sub), own.dtype)] * (width // sub),
        in_specs=[VMEM] * 2,
        out_specs=[VMEM] * (width // sub),
        compiler_params=params(),
        cost_estimate=cost(own.size, 8 * own.size),
        name="merge",
    )(own, theirs)


def grads_kernel(n_tp, rows, hd, base, *refs):
    *ins, out = refs
    tp = lax.axis_index("tp")
    for g in range(len(ins) // n_tp):
        for kt in range(n_tp):
            start = pl.multiple_of(base + lax.bitwise_xor(tp, jnp.int32(kt)) * hd, hd)
            for h in range(n_tp):
                piece = ins[g * n_tp + h][:, pl.ds(start, hd)]
                column = (g * n_tp + kt) * rows
                out[h * hd:(h + 1) * hd, column:column + rows] = piece.T


def grads(pieces, n_tp, hd, base):
    rows = pieces[0].shape[0]
    size = len(pieces) * rows * hd * n_tp
    return pl.pallas_call(
        functools.partial(grads_kernel, n_tp, rows, hd, base),
        out_shape=jax.ShapeDtypeStruct((n_tp * hd, len(pieces) * rows), jnp.bfloat16),
        in_specs=[VMEM] * len(pieces),
        out_specs=VMEM,
        compiler_params=params(),
        cost_estimate=cost(size, 4 * size),
        name="grads",
    )(*pieces)


def matmul_kernel(sub, gt_ref, *refs):
    *ins, mine, theirs = refs
    gt = gt_ref[...]
    x = jnp.concatenate([r[:, :2 * sub] for r in ins], axis=0)
    theirs[...] = jnp.dot(gt, x[:, sub:], preferred_element_type=jnp.float32)
    mine[...] = jnp.dot(gt, x[:, :sub], preferred_element_type=jnp.float32)


def matmul(gt, xs, sub):
    columns, tokens = gt.shape
    return pl.pallas_call(
        functools.partial(matmul_kernel, sub),
        out_shape=[jax.ShapeDtypeStruct((columns, sub), jnp.float32)] * 2,
        in_specs=[VMEM] * (1 + len(xs)),
        out_specs=[VMEM] * 2,
        compiler_params=params(),
        cost_estimate=cost(4 * columns * tokens * sub, 4 * tokens * sub),
        name="matmul",
    )(gt, *xs)


def product_kernel(gt_a, gt_b, *refs):
    *ins, out = refs
    rows = ins[0].shape[0] // 2
    own = jnp.concatenate([r[:rows, :] for r in ins], axis=0)
    theirs = jnp.concatenate([r[rows:, :] for r in ins], axis=0)
    total = jnp.dot(gt_a[...], own, preferred_element_type=jnp.float32)
    total += jnp.dot(gt_b[...], theirs, preferred_element_type=jnp.float32)
    out[...] = total.astype(out.dtype)


def product(gts, xs, dtype):
    columns = gts[0].shape[0]
    sub = xs[0].shape[1]
    size = sum(x.size for x in xs)
    return pl.pallas_call(
        product_kernel,
        out_shape=jax.ShapeDtypeStruct((columns, sub), dtype),
        in_specs=[VMEM] * (2 + len(xs)),
        out_specs=VMEM,
        compiler_params=params(),
        cost_estimate=cost(2 * columns * size, 2 * size),
        name="product",
    )(*gts, *xs)


def join_kernel(*refs):
    *ins, out = refs
    out[...] = sum(r[...].astype(jnp.float32) for r in ins).astype(out.dtype)


def join(*parts):
    a = parts[0]
    return pl.pallas_call(
        join_kernel,
        out_shape=jax.ShapeDtypeStruct(a.shape, jnp.bfloat16),
        in_specs=[VMEM] * len(parts),
        out_specs=VMEM,
        compiler_params=params(),
        cost_estimate=cost(a.size, 10 * a.size),
        name="join",
    )(*parts)


def total_kernel(*refs):
    *ins, own, other, squares = refs
    total = ins[0][...]
    for r in ins[1:]:
        total = total + r[...].astype(jnp.float32)
    half = own.shape[0]
    own[...] = total[:half]
    other[...] = total[half:]
    squared = (total * total).reshape(-1, 8, total.shape[1]).sum(0)
    squares[...] = sum(squared[:, n:n + 128] for n in range(128, squared.shape[1], 128)) + squared[:, :128]


def totals(parts):
    columns, sub = parts[0].shape
    half = jax.ShapeDtypeStruct((columns // 2, sub), jnp.float32)
    return pl.pallas_call(
        total_kernel,
        out_shape=[half, half, jax.ShapeDtypeStruct((8, 128), jnp.float32)],
        in_specs=[VMEM] * len(parts),
        out_specs=[VMEM] * 3,
        compiler_params=params(),
        cost_estimate=cost(8 * columns * sub, 8 * columns * sub),
        name="totals",
    )(*parts)


def clip_kernel(limit_squared, own, other, *refs):
    *squares, out = refs
    tp = lax.axis_index("tp")
    sub = own.shape[1]
    total = jnp.sum(sum(r[...] for r in squares))
    norm = jnp.sqrt(jnp.full((8, 128), total, jnp.float32))
    factor = jnp.minimum(jnp.float32(1.0), jnp.sqrt(jnp.float32(limit_squared)) / norm)[:1]
    out[pl.ds(pl.multiple_of(tp * sub, sub), sub), :] = own[...].T * factor
    out[pl.ds(pl.multiple_of((1 - tp) * sub, sub), sub), :] = other[...].T * factor


def clip(own, other, squares, limit_squared):
    hd, sub = own.shape
    return pl.pallas_call(
        functools.partial(clip_kernel, limit_squared),
        out_shape=jax.ShapeDtypeStruct((2 * sub, hd), jnp.float32),
        in_specs=[VMEM] * (2 + len(squares)),
        out_specs=VMEM,
        compiler_params=params(),
        cost_estimate=cost(4 * hd * sub, 16 * hd * sub),
        name="clip",
    )(own, other, *squares)


FIRST_LIMIT = 54_000_000
INNER = 4


def keys_of(n_tp):
    far = INNER // 2 * n_tp
    return [0] + list(range(1, n_tp)) + [far + k for k in range(n_tp)]


def fast_body(stash_values, stash_scales, value_grad):
    n_dp, n_tp = lax.axis_size("dp"), lax.axis_size("tp")
    count = n_dp * n_tp
    plane = INNER * n_tp
    depth = count // plane
    _, width = stash_values.shape
    sub = width // count
    keys = keys_of(n_tp)
    core = n_tp
    scales = stash_scales.T

    def send(value, distance):
        return lax.ppermute(value, AXES, [(i, i ^ distance) for i in range(count)])

    order = list(range(depth - 1, -1, -1))
    joined = jnp.concatenate([scales, value_grad])
    packed = pack(stash_values, joined, n_tp, plane, order[:1], keys, core, sub, value_grad)
    mine, theirs = pack(stash_values, scales, n_tp, plane, order[1:], keys, core, sub)
    packed += merge(mine, send(theirs, core), sub)
    terms = []
    for n, j in enumerate(order):
        own, *away = packed[n * len(keys):(n + 1) * len(keys)]
        arrived = [own] + [send(v, k) for k, v in zip(keys[1:], away)]
        if n == 0:
            gt = grads(arrived, n_tp, value_grad.shape[1], 2 * sub)
            mine, theirs = matmul(gt, arrived, sub)
            value = join(mine, send(theirs, core))
            gts = [gt, send(gt, core)]
        else:
            value = product(gts, arrived, jnp.bfloat16 if j else jnp.float32)
        terms.append(send(value, j * plane) if j else value)
    own, other, squares = totals(terms[::-1])
    other = send(other, 1)
    pieces = [squares]
    for group in [(core,), keys[1:], [j * plane for j in range(1, depth)]]:
        merged = sum(pieces[1:], pieces[0])
        pieces = [merged] + [send(merged, k) for k in group]
    columns = value_grad.shape[1] * n_tp
    return clip(own, other, pieces, width * columns)


def block_dequantize(values, scales):
    rows = values.shape[0]
    blocks = scales.shape[1]
    scaled = (
        values.astype(jnp.float32).reshape(rows, blocks, values.shape[1] // blocks)
        * scales.astype(jnp.float32)[:, :, None]
    )
    return scaled.reshape(rows, values.shape[1]).astype(jnp.bfloat16)


def body(stash_values, stash_scales, value_grad):
    width = stash_values.shape[1]
    columns = value_grad.shape[1]
    dp_count = lax.axis_size("dp")
    tp_count = lax.axis_size("tp")
    own_tokens = stash_values.shape[0]
    sub_rows = width // (dp_count * tp_count)
    if tp_count == 2 and dp_count == 16 and sub_rows % 256 == 0 and own_tokens % 128 == 0 and columns == 128:
        return fast_body(stash_values, stash_scales, value_grad)
    inputs = block_dequantize(stash_values, stash_scales)
    inputs = inputs.reshape(own_tokens, dp_count, tp_count, sub_rows)
    features = lax.all_to_all(inputs, "tp", split_axis=2, concat_axis=0, tiled=True)
    features = features.reshape(own_tokens * tp_count, dp_count * sub_rows)
    all_heads = lax.dot_general(
        features,
        lax.all_gather(value_grad, "tp", axis=1, tiled=True),
        (((0,), (0,)), ((), ())),
        preferred_element_type=jnp.float32,
    )
    summed = lax.psum_scatter(all_heads, "dp", scatter_dimension=0, tiled=True)
    local = lax.all_to_all(summed, "tp", split_axis=1, concat_axis=0, tiled=True)
    total = lax.psum(jnp.sum(summed * summed), ("dp", "tp"))
    limit = jnp.sqrt(jnp.float32(width * columns * lax.axis_size("tp")))
    return local * jnp.minimum(jnp.float32(1.0), limit / jnp.sqrt(total))


def solution(mesh):
    placed = (P(("dp", "tp"), None), P(("dp", "tp"), None), P("dp", "tp"))
    return jax.shard_map(body, mesh=mesh, in_specs=placed, out_specs=P("dp", "tp"), check_vma=False)
```

```python
import functools

import jax
import jax.numpy as jnp
from jax import lax
from jax.experimental import pallas as pl
from jax.experimental.pallas import tpu as pltpu
from jax.sharding import PartitionSpec as P


AXES = ("dp", "tp")
VMEM = pl.BlockSpec(memory_space=pltpu.VMEM)


def params(limit=16 * 1024 * 1024):
    return pltpu.CompilerParams(vmem_limit_bytes=limit)


def cost(flops, moved):
    return pl.CostEstimate(flops=flops, bytes_accessed=moved, transcendentals=0)


def dequantize(values, scales, first, sub, block):
    blocks = scales.shape[0]
    row = lax.broadcasted_iota(jnp.int32, (blocks, sub), 0)
    lane = lax.broadcasted_iota(jnp.int32, (blocks, sub), 1) // block
    pick = (row == lane + first).astype(jnp.bfloat16)
    spread = lax.dot_general(scales, pick, (((0,), (0,)), ((), ())), preferred_element_type=jnp.float32)
    return (values.astype(jnp.float32) * spread).astype(jnp.bfloat16)


def pack_kernel(n_tp, plane, planes, keys, core, sub, block, load, x_ref, s_ref, *refs):
    index = lax.axis_index("dp") * n_tp + lax.axis_index("tp")
    base = 0
    if load:
        g_ref, *outs = refs
        (j,) = planes
        base = lax.bitwise_xor(index, jnp.int32(j * plane)) // plane * plane
        rows, hd = x_ref.shape[0], g_ref.shape[1]
        for out in outs:
            for h in range(n_tp):
                out[:, 2 * sub + h * hd:2 * sub + (h + 1) * hd] = g_ref[h * rows:(h + 1) * rows, :]
    else:
        outs = refs
    scales = s_ref[...]
    for n, j in enumerate(planes):
        for m, key in enumerate(keys):
            for h in range(2):
                part = lax.bitwise_xor(index, jnp.int32((j * plane + key) ^ (h * core)))
                values = x_ref[:, pl.ds(pl.multiple_of((part - base) * sub, sub), sub)]
                values = dequantize(values, scales, part * (sub // block), sub, block)
                if load:
                    outs[m][:, h * sub:(h + 1) * sub] = values
                else:
                    column = (n * len(keys) + m) * sub
                    outs[h][:, column:column + sub] = values


def load_kernel(n_tp, plane, width, j, x_ref, out, sem):
    index = lax.axis_index("dp") * n_tp + lax.axis_index("tp")
    base = lax.bitwise_xor(index, jnp.int32(j * plane)) // plane * width
    copy = pltpu.make_async_copy(x_ref.at[:, pl.ds(pl.multiple_of(base, width), width)], out, sem)
    copy.start()
    copy.wait()


def load_plane(x, n_tp, plane, width, j):
    return pl.pallas_call(
        functools.partial(load_kernel, n_tp, plane, width, j),
        out_shape=jax.ShapeDtypeStruct((x.shape[0], width), x.dtype),
        in_specs=[pl.BlockSpec(memory_space=pltpu.HBM)],
        out_specs=VMEM,
        scratch_shapes=[pltpu.SemaphoreType.DMA],
        compiler_params=params(FIRST_LIMIT),
        cost_estimate=cost(1000 * x.size, 4 * x.size),
        name="load",
    )(x)


def pack(x, scales, n_tp, plane, planes, keys, core, sub, block, *load):
    rows = x.shape[0]
    extra = load[0].size // rows if load else 0
    outs = len(keys) if load else 2
    width = 2 * sub + extra if load else len(planes) * len(keys) * sub
    return pl.pallas_call(
        functools.partial(pack_kernel, n_tp, plane, planes, keys, core, sub, block, bool(load)),
        out_shape=[jax.ShapeDtypeStruct((rows, width), jnp.bfloat16)] * outs,
        in_specs=[VMEM] * (2 + len(load)),
        out_specs=[VMEM] * outs,
        compiler_params=params(),
        cost_estimate=cost(2 * rows * width * outs, 4 * rows * width * outs),
        name="pack",
    )(x, scales, *load)


def merge_kernel(own, theirs, *outs):
    rows = own.shape[0]
    sub = outs[0].shape[1]
    for n, out in enumerate(outs):
        out[:rows, :] = own[:, n * sub:(n + 1) * sub]
        out[rows:, :] = theirs[:, n * sub:(n + 1) * sub]


def merge(own, theirs, sub):
    rows, width = own.shape
    return pl.pallas_call(
        merge_kernel,
        out_shape=[jax.ShapeDtypeStruct((2 * rows, sub), own.dtype)] * (width // sub),
        in_specs=[VMEM] * 2,
        out_specs=[VMEM] * (width // sub),
        compiler_params=params(),
        cost_estimate=cost(own.size, 8 * own.size),
        name="merge",
    )(own, theirs)


def grads_kernel(n_tp, rows, hd, base, *refs):
    *ins, out = refs
    tp = lax.axis_index("tp")
    for g in range(len(ins) // n_tp):
        for kt in range(n_tp):
            start = pl.multiple_of(base + lax.bitwise_xor(tp, jnp.int32(kt)) * hd, hd)
            for h in range(n_tp):
                piece = ins[g * n_tp + h][:, pl.ds(start, hd)]
                column = (g * n_tp + kt) * rows
                out[h * hd:(h + 1) * hd, column:column + rows] = piece.T


def grads(pieces, n_tp, hd, base):
    rows = pieces[0].shape[0]
    size = len(pieces) * rows * hd * n_tp
    return pl.pallas_call(
        functools.partial(grads_kernel, n_tp, rows, hd, base),
        out_shape=jax.ShapeDtypeStruct((n_tp * hd, len(pieces) * rows), jnp.bfloat16),
        in_specs=[VMEM] * len(pieces),
        out_specs=VMEM,
        compiler_params=params(),
        cost_estimate=cost(size, 4 * size),
        name="grads",
    )(*pieces)


def matmul_kernel(sub, gt_ref, *refs):
    *ins, mine, theirs = refs
    gt = gt_ref[...]
    x = jnp.concatenate([r[:, :2 * sub] for r in ins], axis=0)
    theirs[...] = jnp.dot(gt, x[:, sub:], preferred_element_type=jnp.float32)
    mine[...] = jnp.dot(gt, x[:, :sub], preferred_element_type=jnp.float32)


def matmul(gt, xs, sub):
    columns, tokens = gt.shape
    return pl.pallas_call(
        functools.partial(matmul_kernel, sub),
        out_shape=[jax.ShapeDtypeStruct((columns, sub), jnp.float32)] * 2,
        in_specs=[VMEM] * (1 + len(xs)),
        out_specs=[VMEM] * 2,
        compiler_params=params(),
        cost_estimate=cost(4 * columns * tokens * sub, 4 * tokens * sub),
        name="matmul",
    )(gt, *xs)


def product_kernel(gt_a, gt_b, *refs):
    *ins, out = refs
    rows = ins[0].shape[0] // 2
    own = jnp.concatenate([r[:rows, :] for r in ins], axis=0)
    theirs = jnp.concatenate([r[rows:, :] for r in ins], axis=0)
    total = jnp.dot(gt_a[...], own, preferred_element_type=jnp.float32)
    total += jnp.dot(gt_b[...], theirs, preferred_element_type=jnp.float32)
    out[...] = total.astype(out.dtype)


def product(gts, xs, dtype):
    columns = gts[0].shape[0]
    sub = xs[0].shape[1]
    size = sum(x.size for x in xs)
    return pl.pallas_call(
        product_kernel,
        out_shape=jax.ShapeDtypeStruct((columns, sub), dtype),
        in_specs=[VMEM] * (2 + len(xs)),
        out_specs=VMEM,
        compiler_params=params(),
        cost_estimate=cost(2 * columns * size, 2 * size),
        name="product",
    )(*gts, *xs)


def join_kernel(*refs):
    *ins, out = refs
    out[...] = sum(r[...].astype(jnp.float32) for r in ins).astype(out.dtype)


def join(*parts):
    a = parts[0]
    return pl.pallas_call(
        join_kernel,
        out_shape=jax.ShapeDtypeStruct(a.shape, jnp.bfloat16),
        in_specs=[VMEM] * len(parts),
        out_specs=VMEM,
        compiler_params=params(),
        cost_estimate=cost(a.size, 10 * a.size),
        name="join",
    )(*parts)


def total_kernel(*refs):
    *ins, own, other, squares = refs
    total = ins[0][...]
    for r in ins[1:]:
        total = total + r[...].astype(jnp.float32)
    half = own.shape[0]
    own[...] = total[:half]
    other[...] = total[half:]
    squared = (total * total).reshape(-1, 8, total.shape[1]).sum(0)
    squares[...] = sum(squared[:, n:n + 128] for n in range(128, squared.shape[1], 128)) + squared[:, :128]


def totals(parts):
    columns, sub = parts[0].shape
    half = jax.ShapeDtypeStruct((columns // 2, sub), jnp.float32)
    return pl.pallas_call(
        total_kernel,
        out_shape=[half, half, jax.ShapeDtypeStruct((8, 128), jnp.float32)],
        in_specs=[VMEM] * len(parts),
        out_specs=[VMEM] * 3,
        compiler_params=params(),
        cost_estimate=cost(8 * columns * sub, 8 * columns * sub),
        name="totals",
    )(*parts)


def clip_kernel(limit_squared, own, other, *refs):
    *squares, out = refs
    tp = lax.axis_index("tp")
    sub = own.shape[1]
    total = jnp.sum(sum(r[...] for r in squares))
    norm = jnp.sqrt(jnp.full((8, 128), total, jnp.float32))
    factor = jnp.minimum(jnp.float32(1.0), jnp.sqrt(jnp.float32(limit_squared)) / norm)[:1]
    out[pl.ds(pl.multiple_of(tp * sub, sub), sub), :] = own[...].T * factor
    out[pl.ds(pl.multiple_of((1 - tp) * sub, sub), sub), :] = other[...].T * factor


def clip(own, other, squares, limit_squared):
    hd, sub = own.shape
    return pl.pallas_call(
        functools.partial(clip_kernel, limit_squared),
        out_shape=jax.ShapeDtypeStruct((2 * sub, hd), jnp.float32),
        in_specs=[VMEM] * (2 + len(squares)),
        out_specs=VMEM,
        compiler_params=params(),
        cost_estimate=cost(4 * hd * sub, 16 * hd * sub),
        name="clip",
    )(own, other, *squares)


FIRST_LIMIT = 54_000_000
INNER = 4


def keys_of(n_tp):
    far = INNER // 2 * n_tp
    return [0] + list(range(1, n_tp)) + [far + k for k in range(n_tp)]


def fast_body(stash_values, stash_scales, value_grad):
    n_dp, n_tp = lax.axis_size("dp"), lax.axis_size("tp")
    count = n_dp * n_tp
    plane = INNER * n_tp
    depth = count // plane
    _, width = stash_values.shape
    sub = width // count
    keys = keys_of(n_tp)
    core = n_tp
    scales = stash_scales.T

    def send(value, distance):
        return lax.ppermute(value, AXES, [(i, i ^ distance) for i in range(count)])

    order = list(range(depth - 1, -1, -1))
    block = width // scales.shape[0]
    start = load_plane(stash_values, n_tp, plane, plane * sub, order[0])
    packed = pack(start, scales, n_tp, plane, order[:1], keys, core, sub, block, value_grad)
    mine, theirs = pack(stash_values, scales, n_tp, plane, order[1:], keys, core, sub, block)
    packed += merge(mine, send(theirs, core), sub)
    terms = []
    for n, j in enumerate(order):
        own, *away = packed[n * len(keys):(n + 1) * len(keys)]
        arrived = [own] + [send(v, k) for k, v in zip(keys[1:], away)]
        if n == 0:
            gt = grads(arrived, n_tp, value_grad.shape[1], 2 * sub)
            mine, theirs = matmul(gt, arrived, sub)
            value = join(mine, send(theirs, core))
            gts = [gt, send(gt, core)]
        else:
            value = product(gts, arrived, jnp.bfloat16 if j else jnp.float32)
        terms.append(send(value, j * plane) if j else value)
    own, other, squares = totals(terms[::-1])
    other = send(other, 1)
    pieces = [squares]
    for group in [(core,), keys[1:], [j * plane for j in range(1, depth)]]:
        merged = sum(pieces[1:], pieces[0])
        pieces = [merged] + [send(merged, k) for k in group]
    columns = value_grad.shape[1] * n_tp
    return clip(own, other, pieces, width * columns)


def block_dequantize(values, scales):
    rows = values.shape[0]
    blocks = scales.shape[1]
    scaled = (
        values.astype(jnp.float32).reshape(rows, blocks, values.shape[1] // blocks)
        * scales.astype(jnp.float32)[:, :, None]
    )
    return scaled.reshape(rows, values.shape[1]).astype(jnp.bfloat16)


def body(stash_values, stash_scales, value_grad):
    width = stash_values.shape[1]
    columns = value_grad.shape[1]
    dp_count = lax.axis_size("dp")
    tp_count = lax.axis_size("tp")
    own_tokens = stash_values.shape[0]
    sub_rows = width // (dp_count * tp_count)
    if tp_count == 2 and dp_count == 16 and sub_rows % 256 == 0 and own_tokens % 128 == 0 and columns == 128:
        return fast_body(stash_values, stash_scales, value_grad)
    inputs = block_dequantize(stash_values, stash_scales)
    inputs = inputs.reshape(own_tokens, dp_count, tp_count, sub_rows)
    features = lax.all_to_all(inputs, "tp", split_axis=2, concat_axis=0, tiled=True)
    features = features.reshape(own_tokens * tp_count, dp_count * sub_rows)
    all_heads = lax.dot_general(
        features,
        lax.all_gather(value_grad, "tp", axis=1, tiled=True),
        (((0,), (0,)), ((), ())),
        preferred_element_type=jnp.float32,
    )
    summed = lax.psum_scatter(all_heads, "dp", scatter_dimension=0, tiled=True)
    local = lax.all_to_all(summed, "tp", split_axis=1, concat_axis=0, tiled=True)
    total = lax.psum(jnp.sum(summed * summed), ("dp", "tp"))
    limit = jnp.sqrt(jnp.float32(width * columns * lax.axis_size("tp")))
    return local * jnp.minimum(jnp.float32(1.0), limit / jnp.sqrt(total))


def solution(mesh):
    placed = (P(("dp", "tp"), None), P(("dp", "tp"), None), P("dp", "tp"))
    return jax.shard_map(body, mesh=mesh, in_specs=placed, out_specs=P("dp", "tp"), check_vma=False)
```
